32 devices in a mesh: blk: 16 (over z, y, core), head: 2 (over x).
Axes of the slice: x: 2, y: 2, z: 4, core: 2. Of those that a mesh axis runs over, the one named last changes fastest.
Arguments:
- queries: bfloat16 [8192, 16, 128], P('blk', 'head'), may hold values from -6 to 6
- out_grad: bfloat16 [8192, 16, 128], P('blk', 'head'), may hold values from -6 to 6
- outputs: bfloat16 [8192, 16, 128], P('blk', 'head'), may hold values from -6 to 6
- key_vectors: bfloat16 [8192, 128], P('blk'), may hold values from -6 to 6
- value_vectors: bfloat16 [8192, 128], P('blk'), may hold values from -6 to 6
- logsumexp: float32 [8192, 16], P('blk', 'head'), may hold values from 4 to 7
- positions: int32 [8192], P('blk'), may hold values from 0 to 8191, as said below
- doc_start: int32 [8192], P('blk'), may hold values from 0 to 8191, as said below
Outputs:
- query_grad: bfloat16 [8192, 16, 128], P('blk', 'head')
- key_grad: bfloat16 [8192, 128], P('blk')
- value_grad: bfloat16 [8192, 128], P('blk')
The draws below stay inside these ranges and needn't reach their ends.
Inputs may be any that keep to these rules, and one draw needn't show every extreme that they name: positions is a permutation of 0 to 8191; row r holds position (r mod 512) * 16 + sigma(r div 512), sigma a permutation of the blocks of 512 rows. doc_start of a row is the first position of the document that holds the row's position; documents are runs of consecutive positions, the first starting at 0, and the last position starts a document of its own.
All inputs are finite; a program needn't handle non-finite values.
Results may differ from the reference program's by a relative error of at most 0.0063.
Values may be sent and summed in bfloat16 or wider, within the bound.
A program may use at most 64 MiB of HBM per device.

```python
import jax
import jax.numpy as jnp
from jax import lax

HQ = 16
HD = 128
TOK_DEV = 512
STEPS = 4
SEQ = 8192
N_BLK = 16


def shared_positions(key):
    sub_key = jax.random.fold_in(key, 11)
    block_order = jax.random.permutation(sub_key, N_BLK).astype(jnp.int32)
    row_ids = jnp.arange(SEQ, dtype=jnp.int32)
    return (row_ids % TOK_DEV * N_BLK + block_order[row_ids // TOK_DEV]).astype(jnp.int32)


def draw_positions(key, part):
    return shared_positions(key)


def draw_doc_start(key, part):
    places = shared_positions(key)
    doc_flags = jax.random.randint(jax.random.fold_in(key, 12), (SEQ,), 0, max(SEQ // 8, 2)) == 0
    cell_ids = jnp.arange(SEQ, dtype=jnp.int32)
    start_marks = jnp.where(doc_flags | (cell_ids == 0) | (cell_ids == SEQ - 1), cell_ids, 0).astype(jnp.int32)
    doc_starts = lax.cummax(start_marks, axis=0)
    return doc_starts[places].astype(jnp.int32)


def levels(key, shape, pieces, least, high):
    level, own = 1.0, jax.random.fold_in(key, 6)
    for axis_at, shards_of in pieces:
        steps = jnp.exp(jax.random.uniform(jax.random.fold_in(own, axis_at), (shards_of,), jnp.float32, least / len(pieces), high / len(pieces)))
        level = level * jnp.repeat(steps, shape[axis_at] // shards_of).reshape([-1 if axis == axis_at else 1 for axis in range(len(shape))])
    return level


def normal_values(rng, extent, width, reach, cuts=(), kind=jnp.bfloat16):
    result = width * jax.random.normal(rng, extent, jnp.float32)
    if cuts:
        result = result * levels(rng, extent, cuts, -0.22, 0.18)
    return jnp.clip(result, -reach, reach).astype(kind)


def setup_inputs(seed: int = 0) -> dict:
    key_of = jax.random.split(jax.random.key(seed), 9)
    return {
        "queries": normal_values(key_of[0], (SEQ, HQ, HD), 1.0, 6.0, ((0, 16), (1, 2))),
        "out_grad": normal_values(key_of[1], (SEQ, HQ, HD), 1.0, 6.0, ((0, 16), (1, 2))),
        "outputs": normal_values(key_of[2], (SEQ, HQ, HD), 1.0, 6.0, ((0, 16), (1, 2))),
        "key_vectors": normal_values(key_of[3], (SEQ, HD), 1.0, 6.0, ((0, 16),)),
        "value_vectors": normal_values(key_of[4], (SEQ, HD), 1.0, 6.0, ((0, 16),)),
        "logsumexp": jnp.clip(4.0 + 3.0 * jax.random.uniform(key_of[5], (SEQ, HQ), jnp.float32) ** levels(key_of[5], (SEQ, HQ), ((0, 16), (1, 2)), -0.2, 0.2), 4.0, 7.0),
        "positions": draw_positions(jax.random.fold_in(key_of[8], 71), 0),
        "doc_start": draw_doc_start(jax.random.fold_in(key_of[8], 71), 0),
    }


def block_grads(queries, out_grad, logsumexp, row_delta, query_places, query_starts, key_vectors, value_vectors, key_places):
    scaling = HD ** -0.5
    query_wide = queries.astype(jnp.float32)
    grad_wide = out_grad.astype(jnp.float32)
    key_wide = key_vectors.astype(jnp.float32)
    value_wide = value_vectors.astype(jnp.float32)
    scores = jnp.einsum("thd,kd->htk", query_wide, key_wide) * scaling
    allowed = (key_places[None, :] <= query_places[:, None]) & (key_places[None, :] >= query_starts[:, None])
    attend = jnp.where(allowed[None], jnp.exp(scores - logsumexp.T[:, :, None]), jnp.float32(0.0))
    attend_low = lax.optimization_barrier(attend.astype(jnp.bfloat16)).astype(jnp.float32)
    attend_grad = jnp.einsum("thd,kd->htk", grad_wide, value_wide)
    score_grad = attend * (attend_grad - row_delta.T[:, :, None])
    score_low = lax.optimization_barrier(score_grad.astype(jnp.bfloat16)).astype(jnp.float32)
    value_part = jnp.einsum("htk,thd->kd", attend_low, grad_wide)
    key_part = scaling * jnp.einsum("htk,thd->kd", score_low, query_wide)
    query_part = scaling * jnp.einsum("htk,kd->thd", score_low, key_wide)
    return query_part, key_part, value_part


def reference(queries, out_grad, outputs, key_vectors, value_vectors, logsumexp, positions, doc_start):
    row_delta = jnp.sum(out_grad.astype(jnp.float32) * outputs.astype(jnp.float32), axis=-1)
    query_blocks = queries.reshape(N_BLK, TOK_DEV, HQ, HD)
    grad_blocks = out_grad.reshape(N_BLK, TOK_DEV, HQ, HD)
    norm_blocks = logsumexp.reshape(N_BLK, TOK_DEV, HQ)
    delta_blocks = row_delta.reshape(N_BLK, TOK_DEV, HQ)
    place_blocks = positions.reshape(N_BLK, TOK_DEV)
    start_blocks = doc_start.reshape(N_BLK, TOK_DEV)
    key_blocks = key_vectors.reshape(N_BLK, TOK_DEV, HD)
    value_blocks = value_vectors.reshape(N_BLK, TOK_DEV, HD)
    query_total = jnp.zeros((N_BLK, TOK_DEV, HQ, HD), jnp.float32)
    key_total = jnp.zeros((N_BLK, TOK_DEV, HD), jnp.float32)
    value_total = jnp.zeros((N_BLK, TOK_DEV, HD), jnp.float32)

    def block_pass(inputs):
        return block_grads(*inputs)

    for cycle_step in range(STEPS):
        moved_keys = jnp.roll(key_blocks, -cycle_step, axis=0)
        moved_values = jnp.roll(value_blocks, -cycle_step, axis=0)
        moved_places = jnp.roll(place_blocks, -cycle_step, axis=0)
        query_part, key_part, value_part = lax.map(block_pass, (query_blocks, grad_blocks, norm_blocks, delta_blocks, place_blocks, start_blocks, moved_keys, moved_values, moved_places))
        query_total = query_total + query_part
        key_total = key_total + jnp.roll(key_part, cycle_step, axis=0)
        value_total = value_total + jnp.roll(value_part, cycle_step, axis=0)
    return (query_total.reshape(SEQ, HQ, HD).astype(jnp.bfloat16), key_total.reshape(SEQ, HD).astype(jnp.bfloat16), value_total.reshape(SEQ, HD).astype(jnp.bfloat16))
```

```python
import functools
import math

import jax
import jax.numpy as jnp
from jax import lax
from jax.experimental import pallas as pl
from jax.experimental.pallas import tpu as pltpu
from jax.sharding import PartitionSpec as P

STEPS = 4
TILE = 64
CHUNKS = 4
LOG2E = math.log2(math.e)
MESH = pl.DeviceIdType.MESH
VMEM_SPEC = pl.BlockSpec(memory_space=pltpu.VMEM)


def places(n):
    b = lax.axis_index("blk")
    h = lax.axis_index("head")
    even = lax.rem(b, 2) == 0
    partner = jnp.where(even, b + 1, b - 1)

    def at(d):
        return lax.rem(b + d + n, n)

    return b, h, even, partner, at


def greet(n):
    b, h, even, partner, at = places(n)
    barrier = pltpu.get_barrier_semaphore()
    for d in (-3, -2, -1, 1, 2, 3):
        pl.semaphore_signal(barrier, inc=1, device_id=(at(d), h), device_id_type=MESH)
    pl.semaphore_signal(barrier, inc=1, device_id=(b, 1 - h), device_id_type=MESH)
    pl.semaphore_wait(barrier, 7)


def gather_kernel(n, k_ref, v_ref, pos_ref, kall, vall, pos_all, send, recv, local):
    b, h, even, partner, at = places(n)
    rows = k_ref.shape[0]
    half = rows // 2
    mine = pl.ds(pl.multiple_of(h * half, half), half)
    other = pl.ds(pl.multiple_of((1 - h) * half, half), half)
    pairs = ((k_ref, kall), (v_ref, vall))

    def copy(src, dst, kind, j, who):
        return pltpu.make_async_remote_copy(
            src_ref=src,
            dst_ref=dst,
            send_sem=send.at[kind, j],
            recv_sem=recv.at[kind, j],
            device_id=who,
            device_id_type=MESH,
        )

    own = [
        pltpu.make_async_copy(src, dst.at[0], local.at[j])
        for j, (src, dst) in enumerate(pairs + ((pos_ref, pos_all),))
    ]
    for c in own:
        c.start()
    greet(n)
    pslot = jnp.where(even, 1, 3)
    qslot = jnp.where(even, 3, 1)
    first, third, near = [], [], []
    for j, (src, dst) in enumerate(pairs):
        first.append(copy(src.at[mine], dst.at[2, mine], 0, j, (at(-2), h)))
        third.append(copy(src.at[mine], dst.at[3, mine], 1, j, (at(-3), h)))
        near.append(copy(src, dst.at[1], 2, j, (partner, h)))
    for j in range(2):
        first[j].start()

        @pl.when(even)
        def _():
            third[j].start()

        @pl.when(jnp.logical_not(even))
        def _():
            near[j].start()

    marks = [
        copy(pos_ref, pos_all.at[d], 7 + d // 3, d % 3, (at(-d), h)) for d in range(1, STEPS)
    ]
    for c in marks:
        c.start()

    side, side3, fwd, fwd2 = [], [], [], []
    for j, (src, dst) in enumerate(pairs):
        side.append(copy(dst.at[2, mine], dst.at[2, mine], 3, j, (b, 1 - h)))
        side3.append(copy(dst.at[3, mine], dst.at[3, mine], 4, j, (b, 1 - h)))
        fwd.append(copy(dst.at[2, mine], dst.at[pslot, mine], 5, j, (partner, h)))
        fwd2.append(copy(dst.at[2, other], dst.at[pslot, other], 6, j, (partner, h)))
    for j in range(2):
        first[j].wait_recv()
        side[j].start()
        fwd[j].start()
    for j in range(2):

        @pl.when(jnp.logical_not(even))
        def _():
            third[j].wait_recv()
            side3[j].start()

    for j in range(2):
        side[j].wait_recv()
        fwd2[j].start()
    for j in range(2):
        fwd[j].wait_recv()
        fwd2[j].wait_recv()

        @pl.when(even)
        def _():
            near[j].wait_recv()
            third[j].wait_send()

        @pl.when(jnp.logical_not(even))
        def _():
            side3[j].wait_recv()
            near[j].wait_send()
            side3[j].wait_send()

        first[j].wait_send()
        side[j].wait_send()
        fwd[j].wait_send()
        fwd2[j].wait_send()
    for c in own + marks:
        c.wait()


def gather(n, keys, values, marks):
    rows, width = keys.shape
    shape = jax.ShapeDtypeStruct((STEPS, rows, width), keys.dtype)
    mark = jax.ShapeDtypeStruct((STEPS,) + marks.shape, marks.dtype)
    return pl.pallas_call(
        functools.partial(gather_kernel, n),
        out_shape=(shape, shape, mark),
        in_specs=[VMEM_SPEC] * 3,
        out_specs=(VMEM_SPEC,) * 3,
        scratch_shapes=[
            pltpu.SemaphoreType.DMA((9, 3)),
            pltpu.SemaphoreType.DMA((9, 3)),
            pltpu.SemaphoreType.DMA((3,)),
        ],
        compiler_params=pltpu.CompilerParams(collective_id=0, has_side_effects=True),
        name="gather_kv",
    )(keys, values, marks)


def compute_kernel(
    tile, lo_ref, q_ref, g_ref, rows_ref, span_ref, k_ref, v_ref, kp_ref, dq_ref, dk_ref, dv_ref, dk_acc, dv_acc
):
    i = pl.program_id(0)
    width = q_ref.shape[1]
    scaling = width ** (-0.5)

    @pl.when(i == 0)
    def _():
        dk_acc[...] = jnp.zeros_like(dk_acc)
        dv_acc[...] = jnp.zeros_like(dv_acc)

    q = q_ref[...]
    g = g_ref[...]
    lse = rows_ref[0:1, :]
    delta = rows_ref[1:2, :]
    start = span_ref[0:1, :]
    last = span_ref[1:2, :]
    dq_ref[...] = jnp.zeros_like(dq_ref)
    keys = STEPS * tile
    contract = (((1,), (1,)), ((), ()))

    def body(t, total):
        at = pl.ds(pl.multiple_of(t * tile, tile), tile)
        k = k_ref[:, at, :].reshape(keys, width)
        v = v_ref[:, at, :].reshape(keys, width)
        kp = kp_ref[:, at, :].reshape(keys, 1)
        s = lax.dot_general(k, q, contract, preferred_element_type=jnp.float32)
        ok = (kp <= last) & (kp >= start)
        p = jnp.where(ok, jnp.exp2(s * (scaling * LOG2E) - lse), 0.0)
        dp = lax.dot_general(v, g, contract, preferred_element_type=jnp.float32)
        ds = (p * (dp - delta)).astype(jnp.bfloat16)
        p = p.astype(jnp.bfloat16)
        dv = jnp.dot(p, g, preferred_element_type=jnp.float32)
        dk = jnp.dot(ds, q, preferred_element_type=jnp.float32)
        dv_acc[:, at, :] += dv.reshape(STEPS, tile, width)
        dk_acc[:, at, :] += dk.reshape(STEPS, tile, width)
        return total + lax.dot_general(
            ds, k, (((0,), (0,)), ((), ())), preferred_element_type=jnp.float32
        )

    total = lax.fori_loop(lo_ref[i], i + 1, body, jnp.zeros(q.shape, jnp.float32))
    dq_ref[...] = (total * scaling).astype(dq_ref.dtype)

    @pl.when(i == pl.num_programs(0) - 1)
    def _():
        dk_ref[...] = (dk_acc[...] * scaling).astype(dk_ref.dtype)
        dv_ref[...] = dv_acc[...].astype(dv_ref.dtype)


def compute(tile, lo, q, g, rows, span, kall, vall, kplaces):
    steps, tokens, width = kall.shape
    count = tokens // tile
    block = q.shape[0] // count
    part = jax.ShapeDtypeStruct(kall.shape, jnp.bfloat16)
    whole = lambda i, lo: (0, 0, 0)
    return pl.pallas_call(
        functools.partial(compute_kernel, tile),
        out_shape=(jax.ShapeDtypeStruct(q.shape, q.dtype), part, part),
        grid_spec=pltpu.PrefetchScalarGridSpec(
            num_scalar_prefetch=1,
            grid=(count,),
            in_specs=[
                pl.BlockSpec((block, width), lambda i, lo: (i, 0)),
                pl.BlockSpec((block, width), lambda i, lo: (i, 0)),
                pl.BlockSpec((2, block), lambda i, lo: (0, i)),
                pl.BlockSpec((2, block), lambda i, lo: (0, i)),
                pl.BlockSpec(kall.shape, whole),
                pl.BlockSpec(kall.shape, whole),
                pl.BlockSpec((steps, tokens, 1), whole),
            ],
            out_specs=[
                pl.BlockSpec((block, width), lambda i, lo: (i, 0)),
                pl.BlockSpec(kall.shape, whole),
                pl.BlockSpec(kall.shape, whole),
            ],
            scratch_shapes=[pltpu.VMEM(kall.shape, jnp.float32)] * 2,
        ),
        compiler_params=pltpu.CompilerParams(dimension_semantics=("arbitrary",)),
        name="block_grads",
    )(lo, q, g, rows, span, kall, vall, kplaces)


def reduce_kernel(
    n, pk, pv, ok, ov, near, both, far, mid, total, guest, send, recv
):
    b, h, even, partner, at = places(n)
    rows = pk.shape[1]
    size = rows // CHUNKS
    parts = (pk, pv)
    outs = (ok, ov)
    odd = jnp.logical_not(even)

    def copy(src, dst, kind, j, c, who):
        return pltpu.make_async_remote_copy(
            src_ref=src,
            dst_ref=dst,
            send_sem=send.at[kind, j, c],
            recv_sem=recv.at[kind, j, c],
            device_id=who,
            device_id_type=MESH,
        )

    greet(n)
    work = [(j, c, pl.ds(c * size, size)) for c in range(CHUNKS) for j in range(2)]
    give, own, skip, hop, side = {}, {}, {}, {}, {}
    gslot = jnp.where(even, 3, 1)
    for j, c, r in work:
        give[j, c] = copy(parts[j].at[gslot, r], near.at[j, r], 0, j, c, (partner, h))
        own[j, c] = copy(parts[j].at[1, r], both.at[j, r], 1, j, c, (partner, h))
        skip[j, c] = copy(parts[j].at[3, r], far.at[j, r], 2, j, c, (at(3), h))
        hop[j, c] = copy(mid.at[j, r], guest.at[0, j, r], 3, j, c, (at(2), h))
        side[j, c] = copy(total.at[j, r], guest.at[1, j, r], 4, j, c, (b, 1 - h))
        give[j, c].start()
    for j, c, r in work:
        give[j, c].wait_recv()
        mid[j, r] = (parts[j][2, r].astype(jnp.float32) + near[j, r].astype(jnp.float32)).astype(mid.dtype)
        hop[j, c].start()

        @pl.when(odd)
        def _():
            skip[j, c].start()

        @pl.when(even)
        def _():
            own[j, c].start()

    for j, c, r in work:
        hop[j, c].wait_recv()
        acc = parts[j][0, r].astype(jnp.float32) + guest[0, j, r].astype(jnp.float32)

        @pl.when(even)
        def _():
            skip[j, c].wait_recv()
            total[j, r] = (acc + far[j, r].astype(jnp.float32)).astype(total.dtype)

        @pl.when(odd)
        def _():
            own[j, c].wait_recv()
            total[j, r] = (acc + both[j, r].astype(jnp.float32)).astype(total.dtype)

        side[j, c].start()
    for j, c, r in work:
        side[j, c].wait_recv()
        outs[j][r] = (total[j, r].astype(jnp.float32) + guest[1, j, r].astype(jnp.float32)).astype(ok.dtype)
    for j, c, r in work:
        give[j, c].wait_send()
        hop[j, c].wait_send()
        side[j, c].wait_send()

        @pl.when(odd)
        def _():
            skip[j, c].wait_send()

        @pl.when(even)
        def _():
            own[j, c].wait_send()


def reduce_parts(n, pk, pv):
    steps, rows, width = pk.shape
    out = jax.ShapeDtypeStruct((rows, width), jnp.bfloat16)
    buf = pltpu.VMEM((2, rows, width), jnp.bfloat16)
    return pl.pallas_call(
        functools.partial(reduce_kernel, n),
        out_shape=(out, out),
        in_specs=[VMEM_SPEC] * 2,
        out_specs=(VMEM_SPEC, VMEM_SPEC),
        scratch_shapes=[
            buf,
            buf,
            buf,
            buf,
            buf,
            pltpu.VMEM((2, 2, rows, width), jnp.bfloat16),
            pltpu.SemaphoreType.DMA((5, 2, CHUNKS)),
            pltpu.SemaphoreType.DMA((5, 2, CHUNKS)),
        ],
        compiler_params=pltpu.CompilerParams(collective_id=1, has_side_effects=True),
        name="reduce_parts",
    )(pk, pv)


def on_device(
    n, queries, out_grad, outputs, key_vectors, value_vectors, logsumexp, positions, doc_start
):
    tokens, heads, width = queries.shape
    marks = jnp.broadcast_to(positions[:1], (8, width))
    kall, vall, marks = gather(n, key_vectors, value_vectors, marks)
    row_delta = jnp.sum(out_grad.astype(jnp.float32) * outputs.astype(jnp.float32), axis=-1)
    rows = jnp.stack([(logsumexp * LOG2E).reshape(-1), row_delta.reshape(-1)])
    span = jnp.stack([jnp.repeat(doc_start, heads), jnp.repeat(positions, heads)])
    kplaces = (jnp.arange(tokens, dtype=jnp.int32)[None, :] * n + marks[:, 0, :1])[:, :, None]
    lo = doc_start[::TILE] // n // TILE
    dq, pk, pv = compute(
        TILE,
        lo,
        queries.reshape(-1, width),
        out_grad.reshape(-1, width),
        rows,
        span,
        kall,
        vall,
        kplaces,
    )
    dk, dv = reduce_parts(n, pk, pv)
    return dq.reshape(queries.shape), dk, dv


def solution(mesh):
    n = mesh.shape["blk"]
    in_specs = (
        P("blk", "head", None),
        P("blk", "head", None),
        P("blk", "head", None),
        P("blk", None),
        P("blk", None),
        P("blk", "head"),
        P("blk"),
        P("blk"),
    )
    out_specs = (P("blk", "head", None), P("blk", None), P("blk", None))
    return jax.shard_map(
        functools.partial(on_device, n),
        mesh=mesh,
        in_specs=in_specs,
        out_specs=out_specs,
        check_vma=False,
    )
```

```python
import functools
import math

import jax
import jax.numpy as jnp
from jax import lax
from jax.experimental import pallas as pl
from jax.experimental.pallas import tpu as pltpu
from jax.sharding import PartitionSpec as P

STEPS = 4
TILE = 64
CHUNKS = 4
LOG2E = math.log2(math.e)
MESH = pl.DeviceIdType.MESH
VMEM_SPEC = pl.BlockSpec(memory_space=pltpu.VMEM)


def places(n):
    b = lax.axis_index("blk")
    h = lax.axis_index("head")
    even = lax.rem(b, 2) == 0
    partner = jnp.where(even, b + 1, b - 1)

    def at(d):
        return lax.rem(b + d + n, n)

    return b, h, even, partner, at


def greet(n):
    b, h, even, partner, at = places(n)
    barrier = pltpu.get_barrier_semaphore()
    for d in (-3, -2, -1, 1, 2, 3):
        pl.semaphore_signal(barrier, inc=1, device_id=(at(d), h), device_id_type=MESH)
    pl.semaphore_signal(barrier, inc=1, device_id=(b, 1 - h), device_id_type=MESH)
    pl.semaphore_wait(barrier, 7)


def gather_kernel(
    n, k_ref, v_ref, pos_ref, g_hbm, o_hbm, kall, vall, pos_all, delta, g_ref, o_ref, send, recv, local, wide
):
    b, h, even, partner, at = places(n)
    rows = k_ref.shape[0]
    half = rows // 2
    mine = pl.ds(pl.multiple_of(h * half, half), half)
    other = pl.ds(pl.multiple_of((1 - h) * half, half), half)
    pairs = ((k_ref, kall), (v_ref, vall))

    def copy(src, dst, kind, j, who):
        return pltpu.make_async_remote_copy(
            src_ref=src,
            dst_ref=dst,
            send_sem=send.at[kind, j],
            recv_sem=recv.at[kind, j],
            device_id=who,
            device_id_type=MESH,
        )

    own = [
        pltpu.make_async_copy(src, dst.at[0], local.at[j])
        for j, (src, dst) in enumerate(pairs + ((pos_ref, pos_all),))
    ]
    wides = [
        pltpu.make_async_copy(src, dst, wide.at[j])
        for j, (src, dst) in enumerate(((g_hbm, g_ref), (o_hbm, o_ref)))
    ]
    for c in own + wides:
        c.start()
    greet(n)
    pslot = jnp.where(even, 1, 3)
    qslot = jnp.where(even, 3, 1)
    first, third, near = [], [], []
    for j, (src, dst) in enumerate(pairs):
        first.append(copy(src.at[mine], dst.at[2, mine], 0, j, (at(-2), h)))
        third.append(copy(src.at[mine], dst.at[3, mine], 1, j, (at(-3), h)))
        near.append(copy(src, dst.at[1], 2, j, (partner, h)))
    for j in range(2):
        first[j].start()

        @pl.when(even)
        def _():
            third[j].start()

        @pl.when(jnp.logical_not(even))
        def _():
            near[j].start()

    marks = [
        copy(pos_ref, pos_all.at[d], 7 + d // 3, d % 3, (at(-d), h)) for d in range(1, STEPS)
    ]
    for c in marks:
        c.start()

    for c in wides:
        c.wait()
    block = 512
    ones = jnp.ones((8, g_ref.shape[1]), jnp.bfloat16)
    contract = (((1,), (1,)), ((), ()))
    for c in range(g_ref.shape[0] // block):
        r = pl.ds(c * block, block)
        product = g_ref[r].astype(jnp.float32) * o_ref[r].astype(jnp.float32)
        upper = product.astype(jnp.bfloat16)
        lower = (product - upper.astype(jnp.float32)).astype(jnp.bfloat16)
        delta[:, r] = lax.dot_general(
            ones, upper, contract, preferred_element_type=jnp.float32
        ) + lax.dot_general(ones, lower, contract, preferred_element_type=jnp.float32)

    side, side3, fwd, fwd2 = [], [], [], []
    for j, (src, dst) in enumerate(pairs):
        side.append(copy(dst.at[2, mine], dst.at[2, mine], 3, j, (b, 1 - h)))
        side3.append(copy(dst.at[3, mine], dst.at[3, mine], 4, j, (b, 1 - h)))
        fwd.append(copy(dst.at[2, mine], dst.at[pslot, mine], 5, j, (partner, h)))
        fwd2.append(copy(dst.at[2, other], dst.at[pslot, other], 6, j, (partner, h)))
    for j in range(2):
        first[j].wait_recv()
        side[j].start()
        fwd[j].start()
    for j in range(2):

        @pl.when(jnp.logical_not(even))
        def _():
            third[j].wait_recv()
            side3[j].start()

    for j in range(2):
        side[j].wait_recv()
        fwd2[j].start()
    for j in range(2):
        fwd[j].wait_recv()
        fwd2[j].wait_recv()

        @pl.when(even)
        def _():
            near[j].wait_recv()
            third[j].wait_send()

        @pl.when(jnp.logical_not(even))
        def _():
            side3[j].wait_recv()
            near[j].wait_send()
            side3[j].wait_send()

        first[j].wait_send()
        side[j].wait_send()
        fwd[j].wait_send()
        fwd2[j].wait_send()
    for c in own + marks:
        c.wait()


def gather(n, keys, values, marks, g, o):
    rows, width = keys.shape
    shape = jax.ShapeDtypeStruct((STEPS, rows, width), keys.dtype)
    mark = jax.ShapeDtypeStruct((STEPS,) + marks.shape, marks.dtype)
    return pl.pallas_call(
        functools.partial(gather_kernel, n),
        out_shape=(shape, shape, mark, jax.ShapeDtypeStruct((8, g.shape[0]), jnp.float32)),
        in_specs=[VMEM_SPEC] * 3 + [pl.BlockSpec(memory_space=pl.ANY)] * 2,
        out_specs=(VMEM_SPEC,) * 4,
        scratch_shapes=[
            pltpu.VMEM(g.shape, g.dtype),
            pltpu.VMEM(g.shape, g.dtype),
            pltpu.SemaphoreType.DMA((9, 3)),
            pltpu.SemaphoreType.DMA((9, 3)),
            pltpu.SemaphoreType.DMA((3,)),
            pltpu.SemaphoreType.DMA((2,)),
        ],
        compiler_params=pltpu.CompilerParams(collective_id=0, has_side_effects=True),
        name="gather_kv",
    )(keys, values, marks, g, o)


def compute_kernel(
    n, tile, start_ref, q_ref, g_ref, rows_ref, delta_ref, span_ref, k_ref, v_ref, marks_ref,
    dq_ref, dk_ref, dv_ref, dk_acc, dv_acc, dq_acc, p_buf, ds_buf, kp_buf,
):
    steps, tokens, width = k_ref.shape
    count = tokens // tile
    block = q_ref.shape[0] // count
    keys = steps * tile
    scaling = width ** (-0.5)
    contract = (((1,), (1,)), ((), ()))

    dk_acc[...] = jnp.zeros_like(dk_acc)
    dv_acc[...] = jnp.zeros_like(dv_acc)
    dq_acc[...] = jnp.zeros_like(dq_acc)
    ramp = lax.broadcasted_iota(jnp.int32, (tile, width), 0) * n
    for s in range(steps):
        kp_buf[s * tile : (s + 1) * tile, :] = ramp + marks_ref[s, 0:1, :]

    def lowest(i):
        return start_ref[i * tile] // (n * tile)

    def probs(i, t):
        at = pl.ds(pl.multiple_of(t * tile, tile), tile)
        r = pl.ds(pl.multiple_of(i * block, block), block)
        k = k_ref[:, at, :].reshape(keys, width)
        v = v_ref[:, at, :].reshape(keys, width)
        moved = t * (tile * n)
        start = span_ref[0:1, r] - moved
        last = span_ref[1:2, r] - moved
        kp = jnp.concatenate([kp_buf[...]] * (block // width), axis=1)
        s = lax.dot_general(k, q_ref[r, :], contract, preferred_element_type=jnp.float32)
        dp = lax.dot_general(v, g_ref[r, :], contract, preferred_element_type=jnp.float32)
        ok = (kp <= last) & (kp >= start)
        p = jnp.where(ok, jnp.exp2(s * (scaling * LOG2E) - rows_ref[0:1, r]), 0.0)
        return p.astype(jnp.bfloat16), (p * (dp - delta_ref[0:1, r])).astype(jnp.bfloat16)

    def add_grads(i, t):
        at = pl.ds(pl.multiple_of(t * tile, tile), tile)
        r = pl.ds(pl.multiple_of(i * block, block), block)
        k = k_ref[:, at, :].reshape(keys, width)
        ds = ds_buf[...]
        dv = jnp.dot(p_buf[...], g_ref[r, :], preferred_element_type=jnp.float32)
        dk = jnp.dot(ds, q_ref[r, :], preferred_element_type=jnp.float32)
        dv_acc[:, at, :] += dv.reshape(steps, tile, width)
        dk_acc[:, at, :] += dk.reshape(steps, tile, width)
        dq_acc[r, :] += lax.dot_general(
            ds, k, (((0,), (0,)), ((), ())), preferred_element_type=jnp.float32
        )

    def put(pair):
        p_buf[...], ds_buf[...] = pair

    total = lax.fori_loop(0, count, lambda i, c: c + i - lowest(i) + 1, 0)
    put(probs(0, lowest(0)))

    def body(_, spot):
        i, t = spot
        done = t >= i
        new_i = jnp.where(done, i + 1, i)
        new_t = jnp.where(done, lowest(new_i), t + 1)
        pair = probs(new_i, new_t)
        add_grads(i, t)
        put(pair)
        return new_i, new_t

    i, t = lax.fori_loop(1, total, body, (jnp.int32(0), lowest(0)))
    add_grads(i, t)
    dq_ref[...] = (dq_acc[...] * scaling).astype(dq_ref.dtype)
    dk_ref[...] = (dk_acc[...] * scaling).astype(dk_ref.dtype)
    dv_ref[...] = dv_acc[...].astype(dv_ref.dtype)


def compute(n, tile, starts, q, g, rows, delta, span, kall, vall, marks):
    steps, tokens, width = kall.shape
    block = q.shape[0] // (tokens // tile)
    part = jax.ShapeDtypeStruct(kall.shape, jnp.bfloat16)
    return pl.pallas_call(
        functools.partial(compute_kernel, n, tile),
        out_shape=(jax.ShapeDtypeStruct(q.shape, q.dtype), part, part),
        in_specs=[pl.BlockSpec(memory_space=pltpu.SMEM)] + [VMEM_SPEC] * 8,
        out_specs=(VMEM_SPEC,) * 3,
        scratch_shapes=[
            pltpu.VMEM(kall.shape, jnp.float32),
            pltpu.VMEM(kall.shape, jnp.float32),
            pltpu.VMEM(q.shape, jnp.float32),
            pltpu.VMEM((steps * tile, block), jnp.bfloat16),
            pltpu.VMEM((steps * tile, block), jnp.bfloat16),
            pltpu.VMEM((steps * tile, width), jnp.int32),
        ],
        name="block_grads",
    )(starts, q, g, rows, delta, span, kall, vall, marks)


def reduce_kernel(
    n, pk, pv, total, last, near, both, far, mid, guest, send, recv
):
    b, h, even, partner, at = places(n)
    rows = pk.shape[1]
    size = rows // CHUNKS
    parts = (pk, pv)
    odd = jnp.logical_not(even)

    def copy(src, dst, kind, j, c, who):
        return pltpu.make_async_remote_copy(
            src_ref=src,
            dst_ref=dst,
            send_sem=send.at[kind, j, c],
            recv_sem=recv.at[kind, j, c],
            device_id=who,
            device_id_type=MESH,
        )

    greet(n)
    work = [(j, c, pl.ds(c * size, size)) for c in range(CHUNKS) for j in range(2)]
    give, own, skip, hop, side = {}, {}, {}, {}, {}
    gslot = jnp.where(even, 3, 1)
    for j, c, r in work:
        give[j, c] = copy(parts[j].at[gslot, r], near.at[j, r], 0, j, c, (partner, h))
        own[j, c] = copy(parts[j].at[1, r], both.at[j, r], 1, j, c, (partner, h))
        skip[j, c] = copy(parts[j].at[3, r], far.at[j, r], 2, j, c, (at(3), h))
        hop[j, c] = copy(mid.at[j, r], guest.at[j, r], 3, j, c, (at(2), h))
        side[j, c] = copy(total.at[j, r], last.at[j, r], 4, j, c, (b, 1 - h))
        give[j, c].start()
    for j, c, r in work:
        give[j, c].wait_recv()
        mid[j, r] = (parts[j][2, r].astype(jnp.float32) + near[j, r].astype(jnp.float32)).astype(mid.dtype)
        hop[j, c].start()

        @pl.when(odd)
        def _():
            skip[j, c].start()

        @pl.when(even)
        def _():
            own[j, c].start()

    for j, c, r in work:
        hop[j, c].wait_recv()
        acc = parts[j][0, r].astype(jnp.float32) + guest[j, r].astype(jnp.float32)

        @pl.when(even)
        def _():
            skip[j, c].wait_recv()
            total[j, r] = (acc + far[j, r].astype(jnp.float32)).astype(total.dtype)

        @pl.when(odd)
        def _():
            own[j, c].wait_recv()
            total[j, r] = (acc + both[j, r].astype(jnp.float32)).astype(total.dtype)

        side[j, c].start()
    for j, c, r in work:
        side[j, c].wait_recv()
    for j, c, r in work:
        give[j, c].wait_send()
        hop[j, c].wait_send()
        side[j, c].wait_send()

        @pl.when(odd)
        def _():
            skip[j, c].wait_send()

        @pl.when(even)
        def _():
            own[j, c].wait_send()


def reduce_parts(n, pk, pv):
    steps, rows, width = pk.shape
    out = jax.ShapeDtypeStruct((2, rows, width), jnp.bfloat16)
    buf = pltpu.VMEM((2, rows, width), jnp.bfloat16)
    return pl.pallas_call(
        functools.partial(reduce_kernel, n),
        out_shape=(out, out),
        in_specs=[VMEM_SPEC] * 2,
        out_specs=(VMEM_SPEC, VMEM_SPEC),
        scratch_shapes=[
            buf,
            buf,
            buf,
            buf,
            buf,
            pltpu.SemaphoreType.DMA((5, 2, CHUNKS)),
            pltpu.SemaphoreType.DMA((5, 2, CHUNKS)),
        ],
        compiler_params=pltpu.CompilerParams(collective_id=1, has_side_effects=True),
        name="reduce_parts",
    )(pk, pv)


def on_device(
    n, queries, out_grad, outputs, key_vectors, value_vectors, logsumexp, positions, doc_start
):
    tokens, heads, width = queries.shape
    q = queries.reshape(-1, width)
    g = out_grad.reshape(-1, width)
    marks = jnp.broadcast_to(positions[0], (8, width))
    kall, vall, marks, delta = gather(
        n, key_vectors, value_vectors, marks, g, outputs.reshape(-1, width)
    )
    rows = (logsumexp * LOG2E).reshape(1, -1)
    span = jnp.repeat(jnp.stack([doc_start, positions]), heads, axis=1)
    dq, pk, pv = compute(n, TILE, doc_start, q, g, rows, delta, span, kall, vall, marks)
    total, last = reduce_parts(n, pk, pv)
    both = total.astype(jnp.float32) + last.astype(jnp.float32)
    dk, dv = both.astype(jnp.bfloat16)
    return dq.reshape(queries.shape), dk, dv


def solution(mesh):
    n = mesh.shape["blk"]
    in_specs = (
        P("blk", "head", None),
        P("blk", "head", None),
        P("blk", "head", None),
        P("blk", None),
        P("blk", None),
        P("blk", "head"),
        P("blk"),
        P("blk"),
    )
    out_specs = (P("blk", "head", None), P("blk", None), P("blk", None))
    return jax.shard_map(
        functools.partial(on_device, n),
        mesh=mesh,
        in_specs=in_specs,
        out_specs=out_specs,
        check_vma=False,
    )
```

```python
import functools
import math

import jax
import jax.numpy as jnp
from jax import lax
from jax.experimental import pallas as pl
from jax.experimental.pallas import tpu as pltpu
from jax.sharding import PartitionSpec as P

STEPS = 4
TILE = 64
CHUNKS = 4
LOG2E = math.log2(math.e)
MESH = pl.DeviceIdType.MESH
VMEM_SPEC = pl.BlockSpec(memory_space=pltpu.VMEM)


def places(n):
    b = lax.axis_index("blk")
    h = lax.axis_index("head")
    even = lax.rem(b, 2) == 0
    partner = jnp.where(even, b + 1, b - 1)

    def at(d):
        return lax.rem(b + d + n, n)

    return b, h, even, partner, at


def greet(n):
    b, h, even, partner, at = places(n)
    barrier = pltpu.get_barrier_semaphore()
    for d in (-3, -2, -1, 1, 2, 3):
        pl.semaphore_signal(barrier, inc=1, device_id=(at(d), h), device_id_type=MESH)
    pl.semaphore_signal(barrier, inc=1, device_id=(b, 1 - h), device_id_type=MESH)
    pl.semaphore_wait(barrier, 7)


def gather_kernel(
    n, first_ref, k_ref, v_ref, lse_ref, start_ref, last_ref, g_hbm, o_hbm,
    kall, vall, pos_all, table, g_ref, o_ref, pos_ref, send, recv, local, wide,
):
    b, h, even, partner, at = places(n)
    rows = k_ref.shape[0]
    half = rows // 2
    mine = pl.ds(pl.multiple_of(h * half, half), half)
    other = pl.ds(pl.multiple_of((1 - h) * half, half), half)
    pairs = ((k_ref, kall), (v_ref, vall))

    def copy(src, dst, kind, j, who):
        return pltpu.make_async_remote_copy(
            src_ref=src,
            dst_ref=dst,
            send_sem=send.at[kind, j],
            recv_sem=recv.at[kind, j],
            device_id=who,
            device_id_type=MESH,
        )

    own = [
        pltpu.make_async_copy(src, dst.at[0], local.at[j])
        for j, (src, dst) in enumerate(pairs)
    ]
    wides = [
        pltpu.make_async_copy(src, dst, wide.at[j])
        for j, (src, dst) in enumerate(((g_hbm, g_ref), (o_hbm, o_ref)))
    ]
    pos_ref[...] = jnp.full(pos_ref.shape, first_ref[0], pos_ref.dtype)
    pos_all[0] = jnp.full(pos_ref.shape, first_ref[0], pos_ref.dtype)
    for c in own + wides:
        c.start()
    greet(n)
    pslot = jnp.where(even, 1, 3)
    qslot = jnp.where(even, 3, 1)
    first, third, near = [], [], []
    for j, (src, dst) in enumerate(pairs):
        first.append(copy(src.at[mine], dst.at[2, mine], 0, j, (at(-2), h)))
        third.append(copy(src.at[mine], dst.at[3, mine], 1, j, (at(-3), h)))
        near.append(copy(src, dst.at[1], 2, j, (partner, h)))
    for j in range(2):
        first[j].start()

        @pl.when(even)
        def _():
            third[j].start()

        @pl.when(jnp.logical_not(even))
        def _():
            near[j].start()

    marks = [
        copy(pos_ref, pos_all.at[d], 7 + d // 3, d % 3, (at(-d), h)) for d in range(1, STEPS)
    ]
    for c in marks:
        c.start()

    for c in wides:
        c.wait()
    heads, tokens = lse_ref.shape
    block = TILE * heads
    spread = (
        lax.broadcasted_iota(jnp.int32, (TILE, block), 1) // heads
        == lax.broadcasted_iota(jnp.int32, (TILE, block), 0)
    ).astype(jnp.bfloat16)
    choose = (
        lax.broadcasted_iota(jnp.int32, (heads, block), 1) % heads
        == lax.broadcasted_iota(jnp.int32, (heads, block), 0)
    )

    def spread_whole(values):
        upper = values // 256
        lower = values - upper * 256
        up, low = (
            jnp.dot(
                jnp.broadcast_to(part.astype(jnp.float32), (8, TILE)).astype(jnp.bfloat16),
                spread,
                preferred_element_type=jnp.float32,
            )
            for part in (upper, lower)
        )
        return (up * 256.0 + low)[0:1]

    ones = jnp.ones((8, g_ref.shape[1]), jnp.bfloat16)
    contract = (((1,), (1,)), ((), ()))
    for c in range(g_ref.shape[0] // block):
        r = pl.ds(c * block, block)
        product = g_ref[r].astype(jnp.float32) * o_ref[r].astype(jnp.float32)
        upper = product.astype(jnp.bfloat16)
        lower = (product - upper.astype(jnp.float32)).astype(jnp.bfloat16)
        delta = lax.dot_general(
            ones, upper, contract, preferred_element_type=jnp.float32
        ) + lax.dot_general(ones, lower, contract, preferred_element_type=jnp.float32)
        table[0:1, r] = delta[0:1]
        rest = lse_ref[:, c * TILE : (c + 1) * TILE] * LOG2E
        lse = jnp.zeros((heads, block), jnp.float32)
        for _ in range(3):
            part = rest.astype(jnp.bfloat16)
            rest = rest - part.astype(jnp.float32)
            lse += jnp.dot(part, spread, preferred_element_type=jnp.float32)
        table[1:2, r] = jnp.sum(jnp.where(choose, lse, 0.0), axis=0, keepdims=True)
        at = slice(c * TILE, (c + 1) * TILE)
        table[2:3, r] = spread_whole(start_ref[:, at])
        table[3:4, r] = spread_whole(last_ref[:, at])

    side, side3, fwd, fwd2 = [], [], [], []
    for j, (src, dst) in enumerate(pairs):
        side.append(copy(dst.at[2, mine], dst.at[2, mine], 3, j, (b, 1 - h)))
        side3.append(copy(dst.at[3, mine], dst.at[3, mine], 4, j, (b, 1 - h)))
        fwd.append(copy(dst.at[2, mine], dst.at[pslot, mine], 5, j, (partner, h)))
        fwd2.append(copy(dst.at[2, other], dst.at[pslot, other], 6, j, (partner, h)))
    for j in range(2):
        first[j].wait_recv()
        side[j].start()
        fwd[j].start()
    for j in range(2):

        @pl.when(jnp.logical_not(even))
        def _():
            third[j].wait_recv()
            side3[j].start()

    for j in range(2):
        side[j].wait_recv()
        fwd2[j].start()
    for j in range(2):
        fwd[j].wait_recv()
        fwd2[j].wait_recv()

        @pl.when(even)
        def _():
            near[j].wait_recv()
            third[j].wait_send()

        @pl.when(jnp.logical_not(even))
        def _():
            side3[j].wait_recv()
            near[j].wait_send()
            side3[j].wait_send()

        first[j].wait_send()
        side[j].wait_send()
        fwd[j].wait_send()
        fwd2[j].wait_send()
    for c in own + marks:
        c.wait()


def gather(n, keys, values, logsumexp, positions, doc_start, g, o):
    rows, width = keys.shape
    shape = jax.ShapeDtypeStruct((STEPS, rows, width), keys.dtype)
    mark = (8, width)
    return pl.pallas_call(
        functools.partial(gather_kernel, n),
        out_shape=(
            shape,
            shape,
            jax.ShapeDtypeStruct((STEPS,) + mark, positions.dtype),
            jax.ShapeDtypeStruct((4, g.shape[0]), jnp.float32),
        ),
        in_specs=[pl.BlockSpec(memory_space=pltpu.SMEM)]
        + [VMEM_SPEC] * 5
        + [pl.BlockSpec(memory_space=pltpu.HBM)] * 2,
        out_specs=(VMEM_SPEC,) * 4,
        scratch_shapes=[
            pltpu.VMEM(g.shape, g.dtype),
            pltpu.VMEM(g.shape, g.dtype),
            pltpu.VMEM(mark, positions.dtype),
            pltpu.SemaphoreType.DMA((9, 3)),
            pltpu.SemaphoreType.DMA((9, 3)),
            pltpu.SemaphoreType.DMA((2,)),
            pltpu.SemaphoreType.DMA((2,)),
        ],
        compiler_params=pltpu.CompilerParams(
            collective_id=0, has_side_effects=True, vmem_limit_bytes=16 << 20
        ),
        cost_estimate=pl.CostEstimate(
            flops=32 * g.size, bytes_accessed=16 * g.size, transcendentals=0
        ),
        name="gather_kv",
    )(
        positions,
        keys,
        values,
        logsumexp.T,
        doc_start.reshape(1, -1),
        positions.reshape(1, -1),
        g,
        o,
    )


def compute_kernel(
    n, tile, start_ref, q_ref, g_ref, table, k_ref, v_ref, marks_ref,
    dq_ref, dk_ref, dv_ref, dk_acc, dv_acc, dq_acc, p_buf, ds_buf, kp_buf,
):
    steps, tokens, width = k_ref.shape
    count = tokens // tile
    block = q_ref.shape[0] // count
    keys = steps * tile
    scaling = width ** (-0.5)
    contract = (((1,), (1,)), ((), ()))

    dk_acc[...] = jnp.zeros_like(dk_acc)
    dv_acc[...] = jnp.zeros_like(dv_acc)
    dq_acc[...] = jnp.zeros_like(dq_acc)
    ramp = lax.broadcasted_iota(jnp.int32, (tile, width), 0) * n
    for s in range(steps):
        kp_buf[s * tile : (s + 1) * tile, :] = (
            ramp + marks_ref[s, 0:1, :]
        ).astype(jnp.float32)

    def lowest(i):
        return start_ref[i * tile] // (n * tile)

    def probs(i, t):
        at = pl.ds(pl.multiple_of(t * tile, tile), tile)
        r = pl.ds(pl.multiple_of(i * block, block), block)
        k = k_ref[:, at, :].reshape(keys, width)
        v = v_ref[:, at, :].reshape(keys, width)
        moved = (t * (tile * n)).astype(jnp.float32)
        start = table[2:3, r] - moved
        last = table[3:4, r] - moved
        kp = jnp.concatenate([kp_buf[...]] * (block // width), axis=1)
        s = lax.dot_general(k, q_ref[r, :], contract, preferred_element_type=jnp.float32)
        dp = lax.dot_general(v, g_ref[r, :], contract, preferred_element_type=jnp.float32)
        ok = (kp <= last) & (kp >= start)
        p = jnp.where(ok, jnp.exp2(s * (scaling * LOG2E) - table[1:2, r]), 0.0)
        return p.astype(jnp.bfloat16), (p * (dp - table[0:1, r])).astype(jnp.bfloat16)

    def add_grads(i, t):
        at = pl.ds(pl.multiple_of(t * tile, tile), tile)
        r = pl.ds(pl.multiple_of(i * block, block), block)
        k = k_ref[:, at, :].reshape(keys, width)
        ds = ds_buf[...]
        dv = jnp.dot(p_buf[...], g_ref[r, :], preferred_element_type=jnp.float32)
        dk = jnp.dot(ds, q_ref[r, :], preferred_element_type=jnp.float32)
        dv_acc[:, at, :] += dv.reshape(steps, tile, width)
        dk_acc[:, at, :] += dk.reshape(steps, tile, width)
        dq_acc[r, :] += lax.dot_general(
            ds, k, (((0,), (0,)), ((), ())), preferred_element_type=jnp.float32
        )

    def put(pair):
        p_buf[...], ds_buf[...] = pair

    total = lax.fori_loop(0, count, lambda i, c: c + i - lowest(i) + 1, 0)
    put(probs(0, lowest(0)))

    def body(_, spot):
        i, t = spot
        done = t >= i
        new_i = jnp.where(done, i + 1, i)
        new_t = jnp.where(done, lowest(new_i), t + 1)
        pair = probs(new_i, new_t)
        add_grads(i, t)
        put(pair)
        return new_i, new_t

    i, t = lax.fori_loop(1, total, body, (jnp.int32(0), lowest(0)))
    add_grads(i, t)
    dq_ref[...] = (dq_acc[...] * scaling).astype(dq_ref.dtype)
    dk_ref[...] = (dk_acc[...] * scaling).astype(dk_ref.dtype)
    dv_ref[...] = dv_acc[...].astype(dv_ref.dtype)


def compute(n, tile, starts, q, g, table, kall, vall, marks):
    steps, tokens, width = kall.shape
    block = q.shape[0] // (tokens // tile)
    part = jax.ShapeDtypeStruct(kall.shape, jnp.bfloat16)
    return pl.pallas_call(
        functools.partial(compute_kernel, n, tile),
        out_shape=(jax.ShapeDtypeStruct(q.shape, q.dtype), part, part),
        in_specs=[pl.BlockSpec(memory_space=pltpu.SMEM)] + [VMEM_SPEC] * 6,
        out_specs=(VMEM_SPEC,) * 3,
        scratch_shapes=[
            pltpu.VMEM(kall.shape, jnp.float32),
            pltpu.VMEM(kall.shape, jnp.float32),
            pltpu.VMEM(q.shape, jnp.float32),
            pltpu.VMEM((steps * tile, block), jnp.bfloat16),
            pltpu.VMEM((steps * tile, block), jnp.bfloat16),
            pltpu.VMEM((steps * tile, width), jnp.float32),
        ],
        compiler_params=pltpu.CompilerParams(vmem_limit_bytes=28 << 20),
        cost_estimate=pl.CostEstimate(
            flops=10 * q.shape[0] * steps * tokens * width // 2,
            bytes_accessed=6 * q.size,
            transcendentals=q.shape[0] * steps * tokens // 2,
        ),
        name="block_grads",
    )(starts, q, g, table, kall, vall, marks)


def reduce_kernel(
    n, pk, pv, total_k, total_v, last_k, last_v, near, both, far, mid, guest, send, recv
):
    b, h, even, partner, at = places(n)
    rows = pk.shape[1]
    size = rows // CHUNKS
    parts = (pk, pv)
    total = (total_k, total_v)
    last = (last_k, last_v)
    odd = jnp.logical_not(even)

    def copy(src, dst, kind, j, c, who):
        return pltpu.make_async_remote_copy(
            src_ref=src,
            dst_ref=dst,
            send_sem=send.at[kind, j, c],
            recv_sem=recv.at[kind, j, c],
            device_id=who,
            device_id_type=MESH,
        )

    greet(n)
    work = [(j, c, pl.ds(c * size, size)) for c in range(CHUNKS) for j in range(2)]
    give, own, skip, hop, side = {}, {}, {}, {}, {}
    gslot = jnp.where(even, 3, 1)
    for j, c, r in work:
        give[j, c] = copy(parts[j].at[gslot, r], near.at[j, r], 0, j, c, (partner, h))
        own[j, c] = copy(parts[j].at[1, r], both.at[j, r], 1, j, c, (partner, h))
        skip[j, c] = copy(parts[j].at[3, r], far.at[j, r], 2, j, c, (at(3), h))
        hop[j, c] = copy(mid.at[j, r], guest.at[j, r], 3, j, c, (at(2), h))
        side[j, c] = copy(total[j].at[r], last[j].at[r], 4, j, c, (b, 1 - h))
        give[j, c].start()
    for j, c, r in work:
        give[j, c].wait_recv()
        mid[j, r] = (parts[j][2, r].astype(jnp.float32) + near[j, r].astype(jnp.float32)).astype(mid.dtype)
        hop[j, c].start()

        @pl.when(odd)
        def _():
            skip[j, c].start()

        @pl.when(even)
        def _():
            own[j, c].start()

    for j, c, r in work:
        hop[j, c].wait_recv()
        acc = parts[j][0, r].astype(jnp.float32) + guest[j, r].astype(jnp.float32)

        @pl.when(even)
        def _():
            skip[j, c].wait_recv()
            total[j][r] = (acc + far[j, r].astype(jnp.float32)).astype(mid.dtype)

        @pl.when(odd)
        def _():
            own[j, c].wait_recv()
            total[j][r] = (acc + both[j, r].astype(jnp.float32)).astype(mid.dtype)

        side[j, c].start()
    for j, c, r in work:
        side[j, c].wait_recv()
    for j, c, r in work:
        give[j, c].wait_send()
        hop[j, c].wait_send()
        side[j, c].wait_send()

        @pl.when(odd)
        def _():
            skip[j, c].wait_send()

        @pl.when(even)
        def _():
            own[j, c].wait_send()


def reduce_parts(n, pk, pv):
    steps, rows, width = pk.shape
    out = jax.ShapeDtypeStruct((rows, width), jnp.bfloat16)
    buf = pltpu.VMEM((2, rows, width), jnp.bfloat16)
    return pl.pallas_call(
        functools.partial(reduce_kernel, n),
        out_shape=(out,) * 4,
        in_specs=[VMEM_SPEC] * 2,
        out_specs=(VMEM_SPEC,) * 4,
        scratch_shapes=[
            buf,
            buf,
            buf,
            buf,
            buf,
            pltpu.SemaphoreType.DMA((5, 2, CHUNKS)),
            pltpu.SemaphoreType.DMA((5, 2, CHUNKS)),
        ],
        compiler_params=pltpu.CompilerParams(
            collective_id=1, has_side_effects=True, vmem_limit_bytes=12 << 20
        ),
        name="reduce_parts",
    )(pk, pv)


def on_device(
    n, queries, out_grad, outputs, key_vectors, value_vectors, logsumexp, positions, doc_start
):
    tokens, heads, width = queries.shape
    q = queries.reshape(-1, width)
    g = out_grad.reshape(-1, width)
    kall, vall, marks, table = gather(
        n, key_vectors, value_vectors, logsumexp, positions, doc_start, g, outputs.reshape(-1, width)
    )
    dq, pk, pv = compute(n, TILE, doc_start, q, g, table, kall, vall, marks)
    total_k, total_v, last_k, last_v = reduce_parts(n, pk, pv)
    dk = (total_k.astype(jnp.float32) + last_k.astype(jnp.float32)).astype(jnp.bfloat16)
    dv = (total_v.astype(jnp.float32) + last_v.astype(jnp.float32)).astype(jnp.bfloat16)
    return dq.reshape(queries.shape), dk, dv


def solution(mesh):
    n = mesh.shape["blk"]
    in_specs = (
        P("blk", "head", None),
        P("blk", "head", None),
        P("blk", "head", None),
        P("blk", None),
        P("blk", None),
        P("blk", "head"),
        P("blk"),
        P("blk"),
    )
    out_specs = (P("blk", "head", None), P("blk", None), P("blk", None))
    return jax.shard_map(
        functools.partial(on_device, n),
        mesh=mesh,
        in_specs=in_specs,
        out_specs=out_specs,
        check_vma=False,
    )
```

```python
import functools
import math

import jax
import jax.numpy as jnp
from jax import lax
from jax.experimental import pallas as pl
from jax.experimental.pallas import tpu as pltpu
from jax.sharding import PartitionSpec as P

STEPS = 4
TILE = 64
CHUNKS = 4
LOG2E = math.log2(math.e)
MESH = pl.DeviceIdType.MESH
VMEM_SPEC = pl.BlockSpec(memory_space=pltpu.VMEM)


def places(n):
    b = lax.axis_index("blk")
    h = lax.axis_index("head")
    even = lax.rem(b, 2) == 0
    partner = jnp.where(even, b + 1, b - 1)

    def at(d):
        return lax.rem(b + d + n, n)

    return b, h, even, partner, at


def greet(n):
    b, h, even, partner, at = places(n)
    barrier = pltpu.get_barrier_semaphore()
    for d in (-3, -2, -1, 1, 2, 3):
        pl.semaphore_signal(barrier, inc=1, device_id=(at(d), h), device_id_type=MESH)
    pl.semaphore_signal(barrier, inc=1, device_id=(b, 1 - h), device_id_type=MESH)
    pl.semaphore_wait(barrier, 7)


def gather_kernel(
    n, first_ref, k_ref, v_ref, lse_ref, start_ref, last_ref, g_hbm, o_hbm,
    kall, vall, pos_all, table, g_ref, o_ref, pos_ref, send, recv, local, wide,
):
    b, h, even, partner, at = places(n)
    rows = k_ref.shape[0]
    half = rows // 2
    mine = pl.ds(pl.multiple_of(h * half, half), half)
    other = pl.ds(pl.multiple_of((1 - h) * half, half), half)
    pairs = ((k_ref, kall), (v_ref, vall))

    def copy(src, dst, kind, j, who):
        return pltpu.make_async_remote_copy(
            src_ref=src,
            dst_ref=dst,
            send_sem=send.at[kind, j],
            recv_sem=recv.at[kind, j],
            device_id=who,
            device_id_type=MESH,
        )

    own = [
        pltpu.make_async_copy(src, dst.at[0], local.at[j])
        for j, (src, dst) in enumerate(pairs)
    ]
    wides = [
        pltpu.make_async_copy(src, dst, wide.at[j])
        for j, (src, dst) in enumerate(((g_hbm, g_ref), (o_hbm, o_ref)))
    ]
    pos_ref[...] = jnp.full(pos_ref.shape, first_ref[0], pos_ref.dtype)
    pos_all[0] = jnp.full(pos_ref.shape, first_ref[0], pos_ref.dtype)
    for c in own + wides:
        c.start()
    greet(n)
    pslot = jnp.where(even, 1, 3)
    qslot = jnp.where(even, 3, 1)
    first, third, near = [], [], []
    for j, (src, dst) in enumerate(pairs):
        first.append(copy(src.at[mine], dst.at[2, mine], 0, j, (at(-2), h)))
        third.append(copy(src.at[mine], dst.at[3, mine], 1, j, (at(-3), h)))
        near.append(copy(src, dst.at[1], 2, j, (partner, h)))
    for j in range(2):
        first[j].start()

        @pl.when(even)
        def _():
            third[j].start()

        @pl.when(jnp.logical_not(even))
        def _():
            near[j].start()

    marks = [
        copy(pos_ref, pos_all.at[d], 7 + d // 3, d % 3, (at(-d), h)) for d in range(1, STEPS)
    ]
    for c in marks:
        c.start()

    for c in wides:
        c.wait()
    heads, tokens = lse_ref.shape
    block = TILE * heads
    spread = (
        lax.broadcasted_iota(jnp.int32, (TILE, block), 1) // heads
        == lax.broadcasted_iota(jnp.int32, (TILE, block), 0)
    ).astype(jnp.bfloat16)
    choose = (
        lax.broadcasted_iota(jnp.int32, (heads, block), 1) % heads
        == lax.broadcasted_iota(jnp.int32, (heads, block), 0)
    )

    def spread_whole(values):
        upper = values // 256
        lower = values - upper * 256
        up, low = (
            jnp.dot(
                jnp.broadcast_to(part.astype(jnp.float32), (8, TILE)).astype(jnp.bfloat16),
                spread,
                preferred_element_type=jnp.float32,
            )
            for part in (upper, lower)
        )
        return (up * 256.0 + low)[0:1]

    ones = jnp.ones((8, g_ref.shape[1]), jnp.bfloat16)
    contract = (((1,), (1,)), ((), ()))
    for c in range(g_ref.shape[0] // block):
        r = pl.ds(c * block, block)
        product = g_ref[r].astype(jnp.float32) * o_ref[r].astype(jnp.float32)
        upper = product.astype(jnp.bfloat16)
        lower = (product - upper.astype(jnp.float32)).astype(jnp.bfloat16)
        delta = lax.dot_general(
            ones, upper, contract, preferred_element_type=jnp.float32
        ) + lax.dot_general(ones, lower, contract, preferred_element_type=jnp.float32)
        table[0:1, r] = delta[0:1]
        rest = lse_ref[:, c * TILE : (c + 1) * TILE] * LOG2E
        lse = jnp.zeros((heads, block), jnp.float32)
        for _ in range(3):
            part = rest.astype(jnp.bfloat16)
            rest = rest - part.astype(jnp.float32)
            lse += jnp.dot(part, spread, preferred_element_type=jnp.float32)
        table[1:2, r] = jnp.sum(jnp.where(choose, lse, 0.0), axis=0, keepdims=True)
        at = slice(c * TILE, (c + 1) * TILE)
        table[2:3, r] = spread_whole(start_ref[:, at])
        table[3:4, r] = spread_whole(last_ref[:, at])

    side, side3, fwd, fwd2 = [], [], [], []
    for j, (src, dst) in enumerate(pairs):
        side.append(copy(dst.at[2, mine], dst.at[2, mine], 3, j, (b, 1 - h)))
        side3.append(copy(dst.at[3, mine], dst.at[3, mine], 4, j, (b, 1 - h)))
        fwd.append(copy(dst.at[2, mine], dst.at[pslot, mine], 5, j, (partner, h)))
        fwd2.append(copy(dst.at[2, other], dst.at[pslot, other], 6, j, (partner, h)))
    for j in range(2):
        first[j].wait_recv()
        side[j].start()
        fwd[j].start()
    for j in range(2):

        @pl.when(jnp.logical_not(even))
        def _():
            third[j].wait_recv()
            side3[j].start()

    for j in range(2):
        side[j].wait_recv()
        fwd2[j].start()
    for j in range(2):
        fwd[j].wait_recv()
        fwd2[j].wait_recv()

        @pl.when(even)
        def _():
            near[j].wait_recv()
            third[j].wait_send()

        @pl.when(jnp.logical_not(even))
        def _():
            side3[j].wait_recv()
            near[j].wait_send()
            side3[j].wait_send()

        first[j].wait_send()
        side[j].wait_send()
        fwd[j].wait_send()
        fwd2[j].wait_send()
    for c in own + marks:
        c.wait()


def gather(n, keys, values, logsumexp, positions, doc_start, g, o):
    rows, width = keys.shape
    shape = jax.ShapeDtypeStruct((STEPS, rows, width), keys.dtype)
    mark = (8, width)
    return pl.pallas_call(
        functools.partial(gather_kernel, n),
        out_shape=(
            shape,
            shape,
            jax.ShapeDtypeStruct((STEPS,) + mark, positions.dtype),
            jax.ShapeDtypeStruct((4, g.shape[0]), jnp.float32),
        ),
        in_specs=[pl.BlockSpec(memory_space=pltpu.SMEM)]
        + [VMEM_SPEC] * 5
        + [pl.BlockSpec(memory_space=pltpu.HBM)] * 2,
        out_specs=(VMEM_SPEC,) * 4,
        scratch_shapes=[
            pltpu.VMEM(g.shape, g.dtype),
            pltpu.VMEM(g.shape, g.dtype),
            pltpu.VMEM(mark, positions.dtype),
            pltpu.SemaphoreType.DMA((9, 3)),
            pltpu.SemaphoreType.DMA((9, 3)),
            pltpu.SemaphoreType.DMA((2,)),
            pltpu.SemaphoreType.DMA((2,)),
        ],
        compiler_params=pltpu.CompilerParams(
            collective_id=0, has_side_effects=True
        ),
        cost_estimate=pl.CostEstimate(
            flops=32 * g.size, bytes_accessed=16 * g.size, transcendentals=0
        ),
        name="gather_kv",
    )(
        positions,
        keys,
        values,
        logsumexp.T,
        doc_start.reshape(1, -1),
        positions.reshape(1, -1),
        g,
        o,
    )


def compute_kernel(
    n, tile, start_ref, q_ref, g_ref, table, k_ref, v_ref, marks_ref,
    dq_ref, dk_ref, dv_ref, dk_acc, dv_acc, dq_acc, p_buf, ds_buf, kp_buf,
):
    steps, tokens, width = k_ref.shape
    count = tokens // tile
    block = q_ref.shape[0] // count
    keys = steps * tile
    scaling = width ** (-0.5)
    contract = (((1,), (1,)), ((), ()))

    dk_acc[...] = jnp.zeros_like(dk_acc)
    dv_acc[...] = jnp.zeros_like(dv_acc)
    dq_acc[...] = jnp.zeros_like(dq_acc)
    ramp = lax.broadcasted_iota(jnp.int32, (tile, width), 0) * n
    for s in range(steps):
        kp_buf[s * tile : (s + 1) * tile, :] = (
            ramp + marks_ref[s, 0:1, :]
        ).astype(jnp.float32)

    def lowest(i):
        return start_ref[i * tile] // (n * tile)

    def probs(i, t):
        at = pl.ds(pl.multiple_of(t * tile, tile), tile)
        r = pl.ds(pl.multiple_of(i * block, block), block)
        k = k_ref[:, at, :].reshape(keys, width)
        v = v_ref[:, at, :].reshape(keys, width)
        moved = (t * (tile * n)).astype(jnp.float32)
        start = table[2:3, r] - moved
        last = table[3:4, r] - moved
        kp = jnp.concatenate([kp_buf[...]] * (block // width), axis=1)
        s = lax.dot_general(k, q_ref[r, :], contract, preferred_element_type=jnp.float32)
        dp = lax.dot_general(v, g_ref[r, :], contract, preferred_element_type=jnp.float32)
        ok = (kp <= last) & (kp >= start)
        p = jnp.where(ok, jnp.exp2(s * (scaling * LOG2E) - table[1:2, r]), 0.0)
        return p.astype(jnp.bfloat16), (p * (dp - table[0:1, r])).astype(jnp.bfloat16)

    def add_grads(i, t):
        at = pl.ds(pl.multiple_of(t * tile, tile), tile)
        r = pl.ds(pl.multiple_of(i * block, block), block)
        k = k_ref[:, at, :].reshape(keys, width)
        ds = ds_buf[...]
        dv = jnp.dot(p_buf[...], g_ref[r, :], preferred_element_type=jnp.float32)
        dk = jnp.dot(ds, q_ref[r, :], preferred_element_type=jnp.float32)
        dv_acc[:, at, :] += dv.reshape(steps, tile, width)
        dk_acc[:, at, :] += dk.reshape(steps, tile, width)
        dq_acc[r, :] += lax.dot_general(
            ds, k, (((0,), (0,)), ((), ())), preferred_element_type=jnp.float32
        )

    def put(pair):
        p_buf[...], ds_buf[...] = pair

    total = lax.fori_loop(0, count, lambda i, c: c + i - lowest(i) + 1, 0)
    put(probs(0, lowest(0)))

    def body(_, spot):
        i, t = spot
        done = t >= i
        new_i = jnp.where(done, i + 1, i)
        new_t = jnp.where(done, lowest(new_i), t + 1)
        pair = probs(new_i, new_t)
        add_grads(i, t)
        put(pair)
        return new_i, new_t

    i, t = lax.fori_loop(1, total, body, (jnp.int32(0), lowest(0)))
    add_grads(i, t)
    dq_ref[...] = (dq_acc[...] * scaling).astype(dq_ref.dtype)
    dk_ref[...] = (dk_acc[...] * scaling).astype(dk_ref.dtype)
    dv_ref[...] = dv_acc[...].astype(dv_ref.dtype)


def compute(n, tile, starts, q, g, table, kall, vall, marks):
    steps, tokens, width = kall.shape
    block = q.shape[0] // (tokens // tile)
    part = jax.ShapeDtypeStruct(kall.shape, jnp.bfloat16)
    return pl.pallas_call(
        functools.partial(compute_kernel, n, tile),
        out_shape=(jax.ShapeDtypeStruct(q.shape, q.dtype), part, part),
        in_specs=[pl.BlockSpec(memory_space=pltpu.SMEM)] + [VMEM_SPEC] * 6,
        out_specs=(VMEM_SPEC,) * 3,
        scratch_shapes=[
            pltpu.VMEM(kall.shape, jnp.float32),
            pltpu.VMEM(kall.shape, jnp.float32),
            pltpu.VMEM(q.shape, jnp.float32),
            pltpu.VMEM((steps * tile, block), jnp.bfloat16),
            pltpu.VMEM((steps * tile, block), jnp.bfloat16),
            pltpu.VMEM((steps * tile, width), jnp.float32),
        ],
        compiler_params=pltpu.CompilerParams(),
        cost_estimate=pl.CostEstimate(
            flops=10 * q.shape[0] * steps * tokens * width // 2,
            bytes_accessed=6 * q.size,
            transcendentals=q.shape[0] * steps * tokens // 2,
        ),
        name="block_grads",
    )(starts, q, g, table, kall, vall, marks)


def reduce_kernel(
    n, pk, pv, total_k, total_v, last_k, last_v, near, both, far, mid, guest, send, recv
):
    b, h, even, partner, at = places(n)
    rows = pk.shape[1]
    size = rows // CHUNKS
    parts = (pk, pv)
    total = (total_k, total_v)
    last = (last_k, last_v)
    odd = jnp.logical_not(even)

    def copy(src, dst, kind, j, c, who):
        return pltpu.make_async_remote_copy(
            src_ref=src,
            dst_ref=dst,
            send_sem=send.at[kind, j, c],
            recv_sem=recv.at[kind, j, c],
            device_id=who,
            device_id_type=MESH,
        )

    greet(n)
    work = [(j, c, pl.ds(c * size, size)) for c in range(CHUNKS) for j in range(2)]
    give, own, skip, hop, side = {}, {}, {}, {}, {}
    gslot = jnp.where(even, 3, 1)
    for j, c, r in work:
        give[j, c] = copy(parts[j].at[gslot, r], near.at[j, r], 0, j, c, (partner, h))
        own[j, c] = copy(parts[j].at[1, r], both.at[j, r], 1, j, c, (partner, h))
        skip[j, c] = copy(parts[j].at[3, r], far.at[j, r], 2, j, c, (at(3), h))
        hop[j, c] = copy(mid.at[j, r], guest.at[j, r], 3, j, c, (at(2), h))
        side[j, c] = copy(total[j].at[r], last[j].at[r], 4, j, c, (b, 1 - h))
        give[j, c].start()
    for j, c, r in work:
        give[j, c].wait_recv()
        mid[j, r] = (parts[j][2, r].astype(jnp.float32) + near[j, r].astype(jnp.float32)).astype(mid.dtype)
        hop[j, c].start()

        @pl.when(odd)
        def _():
            skip[j, c].start()

        @pl.when(even)
        def _():
            own[j, c].start()

    for j, c, r in work:
        hop[j, c].wait_recv()
        acc = parts[j][0, r].astype(jnp.float32) + guest[j, r].astype(jnp.float32)

        @pl.when(even)
        def _():
            skip[j, c].wait_recv()
            total[j][r] = (acc + far[j, r].astype(jnp.float32)).astype(mid.dtype)

        @pl.when(odd)
        def _():
            own[j, c].wait_recv()
            total[j][r] = (acc + both[j, r].astype(jnp.float32)).astype(mid.dtype)

        side[j, c].start()
    for j, c, r in work:
        side[j, c].wait_recv()
    for j, c, r in work:
        give[j, c].wait_send()
        hop[j, c].wait_send()
        side[j, c].wait_send()

        @pl.when(odd)
        def _():
            skip[j, c].wait_send()

        @pl.when(even)
        def _():
            own[j, c].wait_send()


def reduce_parts(n, pk, pv):
    steps, rows, width = pk.shape
    out = jax.ShapeDtypeStruct((rows, width), jnp.bfloat16)
    buf = pltpu.VMEM((2, rows, width), jnp.bfloat16)
    return pl.pallas_call(
        functools.partial(reduce_kernel, n),
        out_shape=(out,) * 4,
        in_specs=[VMEM_SPEC] * 2,
        out_specs=(VMEM_SPEC,) * 4,
        scratch_shapes=[
            buf,
            buf,
            buf,
            buf,
            buf,
            pltpu.SemaphoreType.DMA((5, 2, CHUNKS)),
            pltpu.SemaphoreType.DMA((5, 2, CHUNKS)),
        ],
        compiler_params=pltpu.CompilerParams(
            collective_id=1, has_side_effects=True
        ),
        name="reduce_parts",
    )(pk, pv)


def on_device(
    n, queries, out_grad, outputs, key_vectors, value_vectors, logsumexp, positions, doc_start
):
    tokens, heads, width = queries.shape
    q = queries.reshape(-1, width)
    g = out_grad.reshape(-1, width)
    kall, vall, marks, table = gather(
        n, key_vectors, value_vectors, logsumexp, positions, doc_start, g, outputs.reshape(-1, width)
    )
    dq, pk, pv = compute(n, TILE, doc_start, q, g, table, kall, vall, marks)
    total_k, total_v, last_k, last_v = reduce_parts(n, pk, pv)
    dk = (total_k.astype(jnp.float32) + last_k.astype(jnp.float32)).astype(jnp.bfloat16)
    dv = (total_v.astype(jnp.float32) + last_v.astype(jnp.float32)).astype(jnp.bfloat16)
    return dq.reshape(queries.shape), dk, dv


def solution(mesh):
    n = mesh.shape["blk"]
    in_specs = (
        P("blk", "head", None),
        P("blk", "head", None),
        P("blk", "head", None),
        P("blk", None),
        P("blk", None),
        P("blk", "head"),
        P("blk"),
        P("blk"),
    )
    out_specs = (P("blk", "head", None), P("blk", None), P("blk", None))
    return jax.shard_map(
        functools.partial(on_device, n),
        mesh=mesh,
        in_specs=in_specs,
        out_specs=out_specs,
        check_vma=False,
    )
```
